1024 devices in a mesh: fsdp: 32 (over z, x_hi), rep: 32 (over x_lo, y, core).
Axes of the slice: x: 4 (x_hi: 2, x_lo: 2; x = x_hi * 2 + x_lo), y: 8, z: 16, core: 2. Of those that a mesh axis runs over, the one named last changes fastest.
Arguments:
- expert_base_rows: bfloat16 [32, 1536, 4096], P('rep', None, 'fsdp'), may hold values from -6 to 6
- factor_in: bfloat16 [32, 1536, 32], P('rep'), may hold values from -6 to 6
- factor_out: bfloat16 [32, 32, 4096], P('rep', None, 'fsdp'), may hold values from -0.29882812 to 0.29882812
- source_group: int32 [4], replicated, may hold values from 0 to 31
- tp_order: int32 [32], replicated, may hold values from 0 to 31, each once
Outputs:
- rollout_weights: bfloat16 [32, 4, 1536, 4096], P('rep', None, 'fsdp')
The draws below stay inside these ranges and needn't reach their ends.
Inputs may be any that keep to these rules, and one draw needn't show every extreme that they name: source_group[k] is the replica index along rep whose expert fills bucket k; entries may repeat. tp_order is a permutation of the 32 row blocks.
All inputs are finite; a program needn't handle non-finite values.
Results may differ from the reference program's by a relative error of at most 0.001.
Values may be sent and summed in bfloat16 or wider, within the bound.
No kernel may reach another device: no remote copies, remote signals or barrier semaphores. Data moves between devices by JAX's collectives and lax.ppermute only.
A program may use at most 64 MiB of HBM per device.

```python
import jax
import jax.numpy as jnp
from jax import lax

D = 4096
FF = 1536
RANK = 32
PUB = 4
EXPERTS = 32
N_FSDP = 32
N_REP = 32


def set_ends(drawn, own_key, smallest, largest):
    place = [jax.random.randint(jax.random.fold_in(own_key, axis), (), 0, length) for axis, length in enumerate(drawn.shape)]
    widest = drawn.shape.index(max(drawn.shape))
    neighbour = place[:widest] + [(place[widest] + 1) % drawn.shape[widest]] + place[widest + 1:]
    return drawn.at[tuple(place)].set(smallest).at[tuple(neighbour)].set(largest)


def block_scale(stream_key, extent, split, least, largest):
    level, own = 1.0, jax.random.fold_in(stream_key, 6)
    for position, blocks in split:
        heights = jnp.exp(jax.random.uniform(jax.random.fold_in(own, position), (blocks,), jnp.float32, least / len(split), largest / len(split)))
        level = level * jnp.repeat(heights, extent[position] // blocks).reshape([-1 if axis == position else 1 for axis in range(len(extent))])
    return level


def noise(rng, extent, deviation, bound, pieces=(), kind=jnp.bfloat16):
    array = jax.random.normal(rng, extent, jnp.float32) * deviation
    if len(pieces) > 0:
        array = block_scale(rng, extent, pieces, -0.22, 0.18) * array
    return jnp.clip(array, min=-bound, max=bound).astype(kind)


def setup_inputs(seed: int = 0) -> dict:
    splits = jax.random.split(jax.random.key(seed), 6)
    return {
        "expert_base_rows": noise(splits[0], (EXPERTS, FF, D), 1.0, 6.0, ((0, 32), (2, 32))),
        "factor_in": noise(splits[1], (EXPERTS, FF, RANK), 1.0, 6.0, ((0, 32),)),
        "factor_out": noise(splits[2], (EXPERTS, RANK, D), 0.05, 0.29882812, ((0, 32), (2, 32))),
        "source_group": set_ends(jax.random.randint(splits[3], (PUB,), 0, N_REP), jax.random.fold_in(splits[3], 1), 0, N_REP - 1).astype(jnp.int32),
        "tp_order": jax.random.permutation(splits[4], N_FSDP).astype(jnp.int32),
    }


ADAPTER_SCALING = 2.0


def merge_expert(operands):
    weight_matrix, left_factor, right_factor = operands
    adapter_delta = jnp.dot(left_factor, right_factor, preferred_element_type=jnp.float32)
    return (weight_matrix.astype(jnp.float32) + ADAPTER_SCALING * adapter_delta).astype(jnp.bfloat16)


def reference(expert_base_rows, factor_in, factor_out, source_group, tp_order):
    merged_weight = lax.map(merge_expert, (expert_base_rows, factor_in, factor_out))
    chosen = jnp.take(merged_weight, source_group.astype(jnp.int32), axis=0)
    blocked = chosen.reshape(PUB, N_FSDP, FF // N_FSDP, D)
    ordered = jnp.take(blocked, tp_order.astype(jnp.int32), axis=1)
    published = ordered.reshape(PUB, FF, D)
    return jnp.broadcast_to(published[None], (N_REP, PUB, FF, D))
```

```python
import jax
import jax.numpy as jnp
from jax import lax
from jax.sharding import Mesh, PartitionSpec as P

ADAPTER_SCALING = 2.0
CUT = {"z": 16, "xh": 2, "xl": 2, "y": 8, "c": 2}
FSDP, REP, EVERY = ("z", "xh"), ("xl", "y", "c"), ("z", "xh", "xl", "y", "c")
N = 32


def swing(r):
    xl, y, c = r // 16, (r // 2) % 8, r % 2
    return (c * 8 + y) * 2 + xl


def body(base, factor_in, factor_out, source_group, tp_order):
    f = lax.axis_index(FSDP)
    delta = jnp.dot(factor_in[0], factor_out[0], preferred_element_type=jnp.float32)
    merged = (base[0].astype(jnp.float32) + ADAPTER_SCALING * delta).astype(jnp.bfloat16)
    rows, width = merged.shape[0] // N, merged.shape[1]
    order = tp_order.at[f ^ swing(jnp.arange(N))].get(mode="promise_in_bounds")
    blocks = merged.reshape(N, rows, width).at[order].get(mode="promise_in_bounds")
    parts = lax.all_to_all(blocks, REP, split_axis=0, concat_axis=0, tiled=True)
    chosen = parts.at[source_group].get(mode="promise_in_bounds")
    pairs = [(s * N + r, (s ^ swing(r)) * N + r) for s in range(N) for r in range(N)]
    piece = lax.ppermute(chosen, EVERY, pairs)
    copies = jnp.broadcast_to(piece[None], (16, *piece.shape))
    half = lax.all_to_all(copies, ("xl", "y"), split_axis=0, concat_axis=0, tiled=True)
    other = lax.ppermute(half, "c", [(0, 1), (1, 0)])
    c = lax.axis_index("c")
    far = jnp.arange(N) ^ f
    at = (far % 2) * 8 + (far // 2) % 8
    both = jnp.concatenate([half, other], axis=0)
    at = at + 16 * ((far // 16) ^ c)
    wide = both.at[at].get(mode="promise_in_bounds")
    return wide.transpose(1, 2, 0, 3).reshape(1, *piece.shape[:2], N * width)


def solution(mesh):
    fine = Mesh(mesh.devices.reshape(tuple(CUT.values())), tuple(CUT))
    placed = (P(REP, None, FSDP), P(REP, None, None), P(REP, None, FSDP), P(), P())
    return jax.shard_map(
        body, mesh=fine, in_specs=placed, out_specs=P(REP, None, FSDP, None), check_vma=False
    )
```

```python
import jax
import jax.numpy as jnp
import numpy as np
from jax import lax
from jax.sharding import Mesh, PartitionSpec as P

ADAPTER_SCALING = 2.0
CUT = {"z": 16, "xh": 2, "xl": 2, "y": 8, "c": 2}
FSDP, REP = ("z", "xh"), ("xl", "y", "c")
SWING = np.array(
    [[0, 8], [1, 9], [2, 10], [3, 11], [4, 7], [12, 15], [5, 6], [13, 14]], np.int32
)


def body(base, factor_in, factor_out, source_group, tp_order):
    z = lax.axis_index("z")
    rows, width = base.shape[1] // 64, base.shape[2]
    delta = jnp.dot(factor_in[0], factor_out[0], preferred_element_type=jnp.float32)
    merged = (base[0].astype(jnp.float32) + ADAPTER_SCALING * delta).astype(jnp.bfloat16)
    xh, xl, y, c = np.meshgrid(*(np.arange(n) for n in (2, 2, 8, 2)), indexing="ij")
    to = (z ^ jnp.asarray(SWING[y, c].ravel())) * 2 + jnp.asarray(xh.ravel())
    order = tp_order.at[to].get(mode="promise_in_bounds") * 2 + jnp.asarray(xl.ravel())
    halves = merged.reshape(64, rows, width).at[order].get(mode="promise_in_bounds")
    parts = lax.all_to_all(halves, ("xh",) + REP, split_axis=0, concat_axis=0, tiled=True)
    pick = jnp.concatenate([source_group, source_group + 32])
    chosen = parts.at[pick].get(mode="promise_in_bounds")
    pairs = [
        ((s * 8 + y) * 2 + c, ((s ^ int(SWING[y, c])) * 8 + y) * 2 + c)
        for s in range(16)
        for y in range(8)
        for c in range(2)
    ]
    piece = lax.ppermute(chosen, ("z", "y", "c"), pairs)
    copies = jnp.broadcast_to(piece[None], (16, *piece.shape))
    half = lax.all_to_all(copies, ("xl", "y"), split_axis=0, concat_axis=0, tiled=True)
    other = lax.ppermute(half, "c", [(0, 1), (1, 0)])
    core = lax.axis_index("c")
    both = jnp.concatenate([half, other], axis=0).reshape(2, 2, 8, 2, 4, rows, width)
    back = np.zeros((16, 2), np.int32)
    for y in range(8):
        for c in range(2):
            back[SWING[y, c]] = (y, c)
    far = jnp.asarray(back)[jnp.arange(16) ^ z]
    wide = both.transpose(0, 2, 1, 3, 4, 5, 6).reshape(16, 2, 2, 4, rows, width)
    wide = wide.at[(far[:, 1] ^ core) * 8 + far[:, 0]].get(mode="promise_in_bounds")
    return wide.transpose(3, 1, 4, 0, 2, 5).reshape(1, 4, 2 * rows, 32 * width)


def solution(mesh):
    fine = Mesh(mesh.devices.reshape(tuple(CUT.values())), tuple(CUT))
    placed = (P(REP, None, FSDP), P(REP, None, None), P(REP, None, FSDP), P(), P())
    return jax.shard_map(
        body, mesh=fine, in_specs=placed, out_specs=P(REP, None, FSDP, None), check_vma=False
    )
```

```python
import jax
import jax.numpy as jnp
from jax import lax
from jax.experimental import pallas as pl
from jax.experimental.pallas import tpu as pltpu
from jax.sharding import Mesh, PartitionSpec as P

ADAPTER_SCALING = 2.0
CUT = {"z": 16, "xh": 2, "xl": 2, "y": 8, "c": 2}
FSDP, REP = ("z", "xh"), ("xl", "y", "c")
EVERY = FSDP + REP
N = 32
SCALAR = pl.BlockSpec(memory_space=pltpu.SMEM)
FAR = pl.BlockSpec(memory_space=pl.ANY)
LOCAL = pl.BlockSpec(memory_space=pltpu.VMEM)


def swing(r):
    xl, y, c = r // 16, (r // 2) % 8, r % 2
    return (c * 8 + y) * 2 + xl


def merge_kernel(me, tp_order, base, left, right, out, tp, rows_in, a, b, merged, sems, tp_sem):
    step = 384
    parts = [pl.ds(at, step) for at in range(0, base.shape[0], step)]
    moves = [
        pltpu.make_async_copy(left, a, sems.at[0]),
        pltpu.make_async_copy(right, b, sems.at[1]),
    ] + [
        pltpu.make_async_copy(base.at[part], rows_in.at[part], sems.at[2 + i])
        for i, part in enumerate(parts)
    ]
    order = pltpu.make_async_copy(tp_order, tp, tp_sem)
    order.start()
    for move in moves:
        move.start()
    for move in moves[:2]:
        move.wait()
    for part, move in zip(parts, moves[2:]):
        delta = lax.dot_general(
            a[:, part], b[...], (((0,), (0,)), ((), ())), preferred_element_type=jnp.float32
        )
        move.wait()
        wide = rows_in[part, :].astype(jnp.float32) + ADAPTER_SCALING * delta
        merged[part, :] = wide.astype(jnp.bfloat16)
    order.wait()
    rows = out.shape[1]
    for r in range(N):
        at = pl.multiple_of(tp[me[0] ^ swing(r)] * rows, 16)
        out[r] = merged[pl.ds(at, rows), :]


def order_kernel(me, own, other, out, wide, sems):
    width = own.shape[-1]
    for k in range(own.shape[1]):
        for at in range(own.shape[0]):
            code = (at % 8) * 2 + at // 8
            for side, ref in enumerate((own, other)):
                lane = pl.multiple_of((me[side] ^ code) * width, width)
                wide[k, :, pl.ds(lane, width)] = ref[at, k]
        pltpu.make_async_copy(wide.at[k], out.at[k], sems.at[k]).start()
    for k in range(own.shape[1]):
        pltpu.make_async_copy(wide.at[k], out.at[k], sems.at[k]).wait()


def body(base, factor_in, factor_out, source_group, tp_order):
    f, c = lax.axis_index(FSDP), lax.axis_index("c")
    rows, width = base.shape[1] // N, base.shape[2]
    blocks = pl.pallas_call(
        merge_kernel,
        out_shape=jax.ShapeDtypeStruct((N, rows, width), jnp.bfloat16),
        in_specs=[SCALAR] + [FAR] * 4,
        out_specs=LOCAL,
        scratch_shapes=[
            pltpu.SMEM((N,), jnp.int32),
            pltpu.VMEM((N * rows, width), jnp.bfloat16),
            pltpu.VMEM(factor_in.shape[:0:-1], jnp.bfloat16),
            pltpu.VMEM(factor_out.shape[1:], jnp.bfloat16),
            pltpu.VMEM((N * rows, width), jnp.bfloat16),
            pltpu.SemaphoreType.DMA((6,)),
            pltpu.SemaphoreType.DMA(()),
        ],
        name="merge",
    )(f[None], tp_order, base[0], factor_in[0].T, factor_out[0])
    parts = lax.all_to_all(blocks, REP, split_axis=0, concat_axis=0, tiled=True)
    chosen = parts.at[source_group].get(mode="promise_in_bounds")
    pairs = [(s * N + r, (s ^ swing(r)) * N + r) for s in range(N) for r in range(N)]
    piece = lax.ppermute(chosen, EVERY, pairs)
    copies = jnp.broadcast_to(piece[None], (16, *piece.shape))
    half = lax.all_to_all(copies, ("xl", "y"), split_axis=0, concat_axis=0, tiled=True)
    other = lax.ppermute(half, "c", [(0, 1), (1, 0)])
    out = pl.pallas_call(
        order_kernel,
        out_shape=jax.ShapeDtypeStruct((*piece.shape[:2], N * width), jnp.bfloat16),
        in_specs=[SCALAR, LOCAL, LOCAL],
        out_specs=FAR,
        scratch_shapes=[
            pltpu.VMEM((*piece.shape[:2], N * width), jnp.bfloat16),
            pltpu.SemaphoreType.DMA((piece.shape[0],)),
        ],
        compiler_params=pltpu.CompilerParams(vmem_limit_bytes=8 << 20),
        name="order",
    )(jnp.stack([f ^ (c * 16), f ^ ((1 - c) * 16)]), half, other)
    return out[None]


def solution(mesh):
    fine = Mesh(mesh.devices.reshape(tuple(CUT.values())), tuple(CUT))
    placed = (P(REP, None, FSDP), P(REP, None, None), P(REP, None, FSDP), P(), P())
    return jax.shard_map(
        body, mesh=fine, in_specs=placed, out_specs=P(REP, None, FSDP, None), check_vma=False
    )
```

```python
import jax
import jax.numpy as jnp
from jax import lax
from jax.experimental import pallas as pl
from jax.experimental.pallas import tpu as pltpu
from jax.sharding import Mesh, PartitionSpec as P

ADAPTER_SCALING = 2.0
CUT = {"z": 16, "xh": 2, "xl": 2, "y": 8, "c": 2}
FSDP, REP = ("z", "xh"), ("xl", "y", "c")
EVERY = FSDP + REP
N = 32
SCALAR = pl.BlockSpec(memory_space=pltpu.SMEM)
FAR = pl.BlockSpec(memory_space=pl.ANY)
LOCAL = pl.BlockSpec(memory_space=pltpu.VMEM)


NEAR = (0, 1, 2, 3, 4, 5, 6, 7, 8, 9, 10, 12, 22, 24, 25, 26)
CODES = (NEAR, tuple(d for d in range(N) if d not in NEAR))


def swing(r):
    return CODES[r % 2][r // 2]


def merge_kernel(me, tp_order, base, left, right, out, tp, rows_in, a, b, merged, sems, tp_sem):
    step = 384
    parts = [pl.ds(at, step) for at in range(0, base.shape[0], step)]
    moves = [
        pltpu.make_async_copy(left, a, sems.at[0]),
        pltpu.make_async_copy(right, b, sems.at[1]),
    ] + [
        pltpu.make_async_copy(base.at[part], rows_in.at[part], sems.at[2 + i])
        for i, part in enumerate(parts)
    ]
    order = pltpu.make_async_copy(tp_order, tp, tp_sem)
    order.start()
    for move in moves:
        move.start()
    for move in moves[:2]:
        move.wait()
    for part, move in zip(parts, moves[2:]):
        delta = lax.dot_general(
            a[:, part], b[...], (((0,), (0,)), ((), ())), preferred_element_type=jnp.float32
        )
        move.wait()
        wide = rows_in[part, :].astype(jnp.float32) + ADAPTER_SCALING * delta
        merged[part, :] = wide.astype(jnp.bfloat16)
    order.wait()
    rows = out.shape[1]
    for r in range(N):
        at = pl.multiple_of(tp[me[0] ^ swing(r)] * rows, 16)
        out[r] = merged[pl.ds(at, rows), :]


def order_kernel(me, own, other, out, wide, sems):
    width = own.shape[-1]
    for k in range(own.shape[1]):
        for at in range(own.shape[0]):
            for side, ref in enumerate((own, other)):
                lane = pl.multiple_of(me[side, at] * width, width)
                wide[k, :, pl.ds(lane, width)] = ref[at, k]
        pltpu.make_async_copy(wide.at[k], out.at[k], sems.at[k]).start()
    for k in range(own.shape[1]):
        pltpu.make_async_copy(wide.at[k], out.at[k], sems.at[k]).wait()


def body(base, factor_in, factor_out, source_group, tp_order):
    f, c = lax.axis_index(FSDP), lax.axis_index("c")
    rows, width = base.shape[1] // N, base.shape[2]
    blocks = pl.pallas_call(
        merge_kernel,
        out_shape=jax.ShapeDtypeStruct((N, rows, width), jnp.bfloat16),
        in_specs=[SCALAR] + [FAR] * 4,
        out_specs=LOCAL,
        scratch_shapes=[
            pltpu.SMEM((N,), jnp.int32),
            pltpu.VMEM((N * rows, width), jnp.bfloat16),
            pltpu.VMEM(factor_in.shape[:0:-1], jnp.bfloat16),
            pltpu.VMEM(factor_out.shape[1:], jnp.bfloat16),
            pltpu.VMEM((N * rows, width), jnp.bfloat16),
            pltpu.SemaphoreType.DMA((6,)),
            pltpu.SemaphoreType.DMA(()),
        ],
        name="merge",
    )(f[None], tp_order, base[0], factor_in[0].T, factor_out[0])
    parts = lax.all_to_all(blocks, REP, split_axis=0, concat_axis=0, tiled=True)
    chosen = parts.at[source_group].get(mode="promise_in_bounds")
    pairs = [(s * N + r, (s ^ swing(r)) * N + r) for s in range(N) for r in range(N)]
    piece = lax.ppermute(chosen, EVERY, pairs)
    copies = jnp.broadcast_to(piece[None], (16, *piece.shape))
    half = lax.all_to_all(copies, ("xl", "y"), split_axis=0, concat_axis=0, tiled=True)
    other = lax.ppermute(half, "c", [(0, 1), (1, 0)])
    out = pl.pallas_call(
        order_kernel,
        out_shape=jax.ShapeDtypeStruct((*piece.shape[:2], N * width), jnp.bfloat16),
        in_specs=[SCALAR, LOCAL, LOCAL],
        out_specs=FAR,
        scratch_shapes=[
            pltpu.VMEM((*piece.shape[:2], N * width), jnp.bfloat16),
            pltpu.SemaphoreType.DMA((piece.shape[0],)),
        ],
        compiler_params=pltpu.CompilerParams(vmem_limit_bytes=8 << 20),
        name="order",
    )(f ^ jnp.where(c == 0, jnp.array(CODES), jnp.array(CODES[::-1])), half, other)
    return out[None]


def solution(mesh):
    fine = Mesh(mesh.devices.reshape(tuple(CUT.values())), tuple(CUT))
    placed = (P(REP, None, FSDP), P(REP, None, None), P(REP, None, FSDP), P(), P())
    return jax.shard_map(
        body, mesh=fine, in_specs=placed, out_specs=P(REP, None, FSDP, None), check_vma=False
    )
```

```python
import jax
import jax.numpy as jnp
from jax import lax
from jax.experimental import pallas as pl
from jax.experimental.pallas import tpu as pltpu
from jax.sharding import Mesh, PartitionSpec as P

ADAPTER_SCALING = 2.0
CUT = {"z": 16, "xh": 2, "xl": 2, "yh": 2, "yl": 4, "c": 2}
FSDP, REP = ("z", "xh"), ("xl", "yh", "yl", "c")
VISIT = ("yl", "yh", "xl", "c")
EVERY = FSDP + REP
N = 32
SCALAR = pl.BlockSpec(memory_space=pltpu.SMEM)
FAR = pl.BlockSpec(memory_space=pl.ANY)
LOCAL = pl.BlockSpec(memory_space=pltpu.VMEM)


def swing(r):
    xl, y, c = r // 16, (r // 2) % 8, r % 2
    return (c * 8 + y) * 2 + xl


def stop(r):
    xl, yh, yl, c = r // 16, r // 8 % 2, r // 2 % 4, r % 2
    return ((yl * 2 + yh) * 2 + xl) * 2 + c


def merge_kernel(me, tp_order, base, left, right, out, tp, slot, rows_in, a, b, merged, *sems):
    in_sems, out_sems, tp_sem = sems
    step, rows = 384, out.shape[1]
    parts = [pl.ds(at, step) for at in range(0, base.shape[0], step)]
    order = pltpu.make_async_copy(tp_order, tp, tp_sem)
    moves = [
        pltpu.make_async_copy(left, a, in_sems.at[0]),
        pltpu.make_async_copy(right, b, in_sems.at[1]),
    ] + [
        pltpu.make_async_copy(base.at[part], rows_in.at[part], in_sems.at[2 + i])
        for i, part in enumerate(parts)
    ]
    order.start()
    for move in moves:
        move.start()
    order.wait()
    for r in range(N):
        slot[tp[me[0] ^ swing(r)]] = stop(r)
    for move in moves[:2]:
        move.wait()
    sent = []
    for part, move in zip(parts, moves[2:]):
        delta = lax.dot_general(
            a[:, part], b[...], (((0,), (0,)), ((), ())), preferred_element_type=jnp.float32
        )
        move.wait()
        wide = rows_in[part, :].astype(jnp.float32) + ADAPTER_SCALING * delta
        merged[part, :] = wide.astype(jnp.bfloat16)
        for t in range(part.start // rows, (part.start + step) // rows):
            block = merged.at[pl.ds(t * rows, rows)]
            sent.append(pltpu.make_async_copy(block, out.at[slot[t]], out_sems.at[t]))
            sent[-1].start()
    for move in sent:
        move.wait()


def order_kernel(me, pieces, *refs):
    out, wide, sems = refs[-3:]
    width, half = pieces.shape[-1], wide.shape[-1]
    place = pl.ds(pl.multiple_of(me[0] // 16 * half, half), half)
    moves = []
    for k in range(pieces.shape[1]):
        for at in range(pieces.shape[0]):
            code = (at % 8) * 2 + at // 8
            lane = pl.multiple_of((me[0] % 16 ^ code) * width, width)
            wide[k, :, pl.ds(lane, width)] = pieces[at, k]
        moves.append(pltpu.make_async_copy(wide.at[k], out.at[k, :, place], sems.at[k]))
        moves[-1].start()
    for move in moves:
        move.wait()


def order(me, pieces, sofar=None):
    _, buckets, rows, width = pieces.shape
    return pl.pallas_call(
        order_kernel,
        out_shape=jax.ShapeDtypeStruct((buckets, rows, N * width), jnp.bfloat16),
        in_specs=[SCALAR, LOCAL] + [FAR] * (sofar is not None),
        out_specs=FAR,
        scratch_shapes=[
            pltpu.VMEM((buckets, rows, N // 2 * width), jnp.bfloat16),
            pltpu.SemaphoreType.DMA((buckets,)),
        ],
        input_output_aliases={} if sofar is None else {2: 0},
        compiler_params=pltpu.CompilerParams(vmem_limit_bytes=8 << 20),
        name="order",
    )(*([me[None], pieces] if sofar is None else [me[None], pieces, sofar]))


def body(base, factor_in, factor_out, source_group, tp_order):
    f, c = lax.axis_index(FSDP), lax.axis_index("c")
    rows, width = base.shape[1] // N, base.shape[2]
    blocks = pl.pallas_call(
        merge_kernel,
        out_shape=jax.ShapeDtypeStruct((N, rows, width), jnp.bfloat16),
        in_specs=[SCALAR] + [FAR] * 4,
        out_specs=FAR,
        scratch_shapes=[
            pltpu.SMEM((N,), jnp.int32),
            pltpu.SMEM((N,), jnp.int32),
            pltpu.VMEM((N * rows, width), jnp.bfloat16),
            pltpu.VMEM(factor_in.shape[:0:-1], jnp.bfloat16),
            pltpu.VMEM(factor_out.shape[1:], jnp.bfloat16),
            pltpu.VMEM((N * rows, width), jnp.bfloat16),
            pltpu.SemaphoreType.DMA((6,)),
            pltpu.SemaphoreType.DMA((N,)),
            pltpu.SemaphoreType.DMA(()),
        ],
        name="merge",
    )(f[None], tp_order, base[0], factor_in[0].T, factor_out[0])
    parts = lax.all_to_all(blocks, VISIT, split_axis=0, concat_axis=0, tiled=True)
    chosen = parts.at[stop(source_group)].get(mode="promise_in_bounds")
    pairs = [(s * N + r, (s ^ swing(r)) * N + r) for s in range(N) for r in range(N)]
    piece = lax.ppermute(chosen, EVERY, pairs)
    copies = jnp.broadcast_to(piece[None], (16, *piece.shape))
    half = lax.all_to_all(copies, ("xl", "yh", "yl"), split_axis=0, concat_axis=0, tiled=True)
    other = lax.ppermute(half, "c", [(0, 1), (1, 0)])
    out = order(f ^ (c * 16), half)
    out = order(f ^ ((1 - c) * 16), other, out)
    return out[None]


def solution(mesh):
    fine = Mesh(mesh.devices.reshape(tuple(CUT.values())), tuple(CUT))
    placed = (P(REP, None, FSDP), P(REP, None, None), P(REP, None, FSDP), P(), P())
    return jax.shard_map(
        body, mesh=fine, in_specs=placed, out_specs=P(REP, None, FSDP, None), check_vma=False
    )
```

```python
import jax
import jax.numpy as jnp
from jax import lax
from jax.experimental import pallas as pl
from jax.experimental.pallas import tpu as pltpu
from jax.sharding import Mesh, PartitionSpec as P

ADAPTER_SCALING = 2.0
CUT = {"z": 16, "xh": 2, "xl": 2, "yh": 2, "yl": 4, "c": 2}
FSDP, REP = ("z", "xh"), ("xl", "yh", "yl", "c")
VISIT = ("yl", "yh", "xl", "c")
EVERY = FSDP + REP
N = 32
SCALAR = pl.BlockSpec(memory_space=pltpu.SMEM)
FAR = pl.BlockSpec(memory_space=pl.ANY)
LOCAL = pl.BlockSpec(memory_space=pltpu.VMEM)


SWING = (
    (8, 31, 2, 26, 1, 27, 9, 29, 28, 19, 11, 23, 3, 13, 0, 16)
    + (4, 24, 6, 25, 10, 18, 5, 22, 30, 15, 7, 21, 14, 20, 12, 17)
)


def swing(r):
    return SWING[r]


def stop(r):
    xl, yh, yl, c = r // 16, r // 8 % 2, r // 2 % 4, r % 2
    return ((yl * 2 + yh) * 2 + xl) * 2 + c


def merge_kernel(me, tp_order, base, left, right, out, tp, slot, rows_in, a, b, merged, *sems):
    in_sems, out_sems, tp_sem = sems
    step, rows = 384, out.shape[1]
    parts = [pl.ds(at, step) for at in range(0, base.shape[0], step)]
    order = pltpu.make_async_copy(tp_order, tp, tp_sem)
    moves = [
        pltpu.make_async_copy(left, a, in_sems.at[0]),
        pltpu.make_async_copy(right, b, in_sems.at[1]),
    ] + [
        pltpu.make_async_copy(base.at[part], rows_in.at[part], in_sems.at[2 + i])
        for i, part in enumerate(parts)
    ]
    order.start()
    for move in moves:
        move.start()
    order.wait()
    for r in range(N):
        slot[tp[me[0] ^ swing(r)]] = stop(r)
    for move in moves[:2]:
        move.wait()
    sent = []
    for part, move in zip(parts, moves[2:]):
        delta = lax.dot_general(
            a[:, part], b[...], (((0,), (0,)), ((), ())), preferred_element_type=jnp.float32
        )
        move.wait()
        wide = rows_in[part, :].astype(jnp.float32) + ADAPTER_SCALING * delta
        merged[part, :] = wide.astype(jnp.bfloat16)
        for t in range(part.start // rows, (part.start + step) // rows):
            block = merged.at[pl.ds(t * rows, rows)]
            sent.append(pltpu.make_async_copy(block, out.at[slot[t]], out_sems.at[t]))
            sent[-1].start()
    for move in sent:
        move.wait()


def order_kernel(places, pieces, *refs):
    out, sems = refs[-2:]
    width = pieces.shape[-1]
    moves = []
    for at in range(pieces.shape[0]):
        lanes = pl.ds(pl.multiple_of(places[at] * width, width), width)
        moves.append(pltpu.make_async_copy(pieces.at[at], out.at[:, :, lanes], sems.at[at]))
        moves[-1].start()
    for move in moves:
        move.wait()


def order(places, pieces, sofar=None):
    many, buckets, rows, width = pieces.shape
    return pl.pallas_call(
        order_kernel,
        out_shape=jax.ShapeDtypeStruct((buckets, rows, N * width), jnp.bfloat16),
        in_specs=[SCALAR, LOCAL] + [FAR] * (sofar is not None),
        out_specs=FAR,
        scratch_shapes=[pltpu.SemaphoreType.DMA((many,))],
        input_output_aliases={} if sofar is None else {2: 0},
        compiler_params=pltpu.CompilerParams(vmem_limit_bytes=8 << 20),
        name="order",
    )(*([places, pieces] if sofar is None else [places, pieces, sofar]))


def body(base, factor_in, factor_out, source_group, tp_order):
    f, c = lax.axis_index(FSDP), lax.axis_index("c")
    rows, width = base.shape[1] // N, base.shape[2]
    blocks = pl.pallas_call(
        merge_kernel,
        out_shape=jax.ShapeDtypeStruct((N, rows, width), jnp.bfloat16),
        in_specs=[SCALAR] + [FAR] * 4,
        out_specs=FAR,
        scratch_shapes=[
            pltpu.SMEM((N,), jnp.int32),
            pltpu.SMEM((N,), jnp.int32),
            pltpu.VMEM((N * rows, width), jnp.bfloat16),
            pltpu.VMEM(factor_in.shape[:0:-1], jnp.bfloat16),
            pltpu.VMEM(factor_out.shape[1:], jnp.bfloat16),
            pltpu.VMEM((N * rows, width), jnp.bfloat16),
            pltpu.SemaphoreType.DMA((6,)),
            pltpu.SemaphoreType.DMA((N,)),
            pltpu.SemaphoreType.DMA(()),
        ],
        name="merge",
    )(f[None], tp_order, base[0], factor_in[0].T, factor_out[0])
    parts = lax.all_to_all(blocks, VISIT, split_axis=0, concat_axis=0, tiled=True)
    chosen = parts.at[stop(source_group)].get(mode="promise_in_bounds")
    pairs = [(s * N + r, (s ^ swing(r)) * N + r) for s in range(N) for r in range(N)]
    piece = lax.ppermute(chosen, EVERY, pairs)
    copies = jnp.broadcast_to(piece[None], (16, *piece.shape))
    half = lax.all_to_all(copies, ("xl", "yh", "yl"), split_axis=0, concat_axis=0, tiled=True)
    other = lax.ppermute(half, "c", [(0, 1), (1, 0)])
    codes = jnp.array((SWING[::2], SWING[1::2]))
    out = order(f ^ jnp.where(c == 0, codes[0], codes[1]), half)
    out = order(f ^ jnp.where(c == 0, codes[1], codes[0]), other, out)
    return out[None]


def solution(mesh):
    fine = Mesh(mesh.devices.reshape(tuple(CUT.values())), tuple(CUT))
    placed = (P(REP, None, FSDP), P(REP, None, None), P(REP, None, FSDP), P(), P())
    return jax.shard_map(
        body, mesh=fine, in_specs=placed, out_specs=P(REP, None, FSDP, None), check_vma=False
    )
```

```python
import jax
import jax.numpy as jnp
from jax import lax
from jax.experimental import pallas as pl
from jax.experimental.pallas import tpu as pltpu
from jax.sharding import Mesh, PartitionSpec as P

ADAPTER_SCALING = 2.0
CUT = {"z": 16, "xh": 2, "xl": 2, "yh": 2, "yl": 4, "c": 2}
FSDP, REP = ("z", "xh"), ("xl", "yh", "yl", "c")
VISIT = ("yl", "yh", "xl", "c")
EVERY = FSDP + REP
N = 32
SCALAR = pl.BlockSpec(memory_space=pltpu.SMEM)
FAR = pl.BlockSpec(memory_space=pl.ANY)
LOCAL = pl.BlockSpec(memory_space=pltpu.VMEM)


LOW = (2, 4, 3, 5, 7, 1, 6, 0)


def swing(r):
    xl, y, c = r // 16, (r // 2) % 8, r % 2
    return (c * 8 + LOW[y]) * 2 + xl


def stop(r):
    xl, yh, yl, c = r // 16, r // 8 % 2, r // 2 % 4, r % 2
    return ((yl * 2 + yh) * 2 + xl) * 2 + c


def merge_kernel(me, tp_order, base, left, right, out, tp, slot, rows_in, a, b, merged, *sems):
    in_sems, out_sems, tp_sem = sems
    step, rows = 384, out.shape[1]
    parts = [pl.ds(at, step) for at in range(0, base.shape[0], step)]
    order = pltpu.make_async_copy(tp_order, tp, tp_sem)
    moves = [
        pltpu.make_async_copy(left, a, in_sems.at[0]),
        pltpu.make_async_copy(right, b, in_sems.at[1]),
    ] + [
        pltpu.make_async_copy(base.at[part], rows_in.at[part], in_sems.at[2 + i])
        for i, part in enumerate(parts)
    ]
    order.start()
    for move in moves:
        move.start()
    order.wait()
    for r in range(N):
        slot[tp[me[0] ^ swing(r)]] = stop(r)
    for move in moves[:2]:
        move.wait()
    sent = []
    for part, move in zip(parts, moves[2:]):
        delta = lax.dot_general(
            a[:, part], b[...], (((0,), (0,)), ((), ())), preferred_element_type=jnp.float32
        )
        move.wait()
        wide = rows_in[part, :].astype(jnp.float32) + ADAPTER_SCALING * delta
        merged[part, :] = wide.astype(jnp.bfloat16)
        for t in range(part.start // rows, (part.start + step) // rows):
            block = merged.at[pl.ds(t * rows, rows)]
            sent.append(pltpu.make_async_copy(block, out.at[slot[t]], out_sems.at[t]))
            sent[-1].start()
    for move in sent:
        move.wait()


def order_kernel(me, pieces, *refs):
    out, wide, sems = refs[-3:]
    width, half = pieces.shape[-1], wide.shape[-1]
    place = pl.ds(pl.multiple_of(me[0] // 16 * half, half), half)
    moves = []
    for k in range(pieces.shape[1]):
        for at in range(pieces.shape[0]):
            code = LOW[at % 8] * 2 + at // 8
            lane = pl.multiple_of((me[0] % 16 ^ code) * width, width)
            wide[k, :, pl.ds(lane, width)] = pieces[at, k]
        moves.append(pltpu.make_async_copy(wide.at[k], out.at[k, :, place], sems.at[k]))
        moves[-1].start()
    for move in moves:
        move.wait()


def order(me, pieces, sofar=None):
    _, buckets, rows, width = pieces.shape
    return pl.pallas_call(
        order_kernel,
        out_shape=jax.ShapeDtypeStruct((buckets, rows, N * width), jnp.bfloat16),
        in_specs=[SCALAR, LOCAL] + [FAR] * (sofar is not None),
        out_specs=FAR,
        scratch_shapes=[
            pltpu.VMEM((buckets, rows, N // 2 * width), jnp.bfloat16),
            pltpu.SemaphoreType.DMA((buckets,)),
        ],
        input_output_aliases={} if sofar is None else {2: 0},
        compiler_params=pltpu.CompilerParams(vmem_limit_bytes=8 << 20),
        name="order",
    )(*([me[None], pieces] if sofar is None else [me[None], pieces, sofar]))


def body(base, factor_in, factor_out, source_group, tp_order):
    f, c = lax.axis_index(FSDP), lax.axis_index("c")
    rows, width = base.shape[1] // N, base.shape[2]
    blocks = pl.pallas_call(
        merge_kernel,
        out_shape=jax.ShapeDtypeStruct((N, rows, width), jnp.bfloat16),
        in_specs=[SCALAR] + [FAR] * 4,
        out_specs=FAR,
        scratch_shapes=[
            pltpu.SMEM((N,), jnp.int32),
            pltpu.SMEM((N,), jnp.int32),
            pltpu.VMEM((N * rows, width), jnp.bfloat16),
            pltpu.VMEM(factor_in.shape[:0:-1], jnp.bfloat16),
            pltpu.VMEM(factor_out.shape[1:], jnp.bfloat16),
            pltpu.VMEM((N * rows, width), jnp.bfloat16),
            pltpu.SemaphoreType.DMA((6,)),
            pltpu.SemaphoreType.DMA((N,)),
            pltpu.SemaphoreType.DMA(()),
        ],
        name="merge",
    )(f[None], tp_order, base[0], factor_in[0].T, factor_out[0])
    parts = lax.all_to_all(blocks, VISIT, split_axis=0, concat_axis=0, tiled=True)
    chosen = parts.at[stop(source_group)].get(mode="promise_in_bounds")
    pairs = [(s * N + r, (s ^ swing(r)) * N + r) for s in range(N) for r in range(N)]
    piece = lax.ppermute(chosen, EVERY, pairs)
    copies = jnp.broadcast_to(piece[None], (16, *piece.shape))
    half = lax.all_to_all(copies, ("xl", "yh", "yl"), split_axis=0, concat_axis=0, tiled=True)
    other = lax.ppermute(half, "c", [(0, 1), (1, 0)])
    out = order(f ^ (c * 16), half)
    out = order(f ^ ((1 - c) * 16), other, out)
    return out[None]


def solution(mesh):
    fine = Mesh(mesh.devices.reshape(tuple(CUT.values())), tuple(CUT))
    placed = (P(REP, None, FSDP), P(REP, None, None), P(REP, None, FSDP), P(), P())
    return jax.shard_map(
        body, mesh=fine, in_specs=placed, out_specs=P(REP, None, FSDP, None), check_vma=False
    )
```
